32 devices in a mesh: expert: 8 (over z, x), shard: 4 (over y, core).
Axes of the slice: x: 2, y: 2, z: 4, core: 2. Of those that a mesh axis runs over, the one named last changes fastest.
Arguments:
- train_down: float32 [16, 6400, 4096], P('expert', None, 'shard'), may hold values from -0.109375 to 0.109375
- router_weight: float32 [4096, 16], P('shard', 'expert'), may hold values from -0.09375 to 0.09375
- router_gain: float32 [4096], P('shard'), may hold values from 0.25 to 1.75
Outputs:
- ready_down: bfloat16 [16, 6400, 4096], P('expert', 'shard')
- scale_down: float32 [16, 6400], P('expert', 'shard')
- serve_router: bfloat16 [4096, 16], replicated
The draws below stay inside these ranges and needn't reach their ends.
All inputs are finite; a program needn't handle non-finite values. Where the reference program divides by a largest or mean magnitude, that divisor is 1e-20 or more.
Results may differ from the reference program's by a relative error of at most 0.001.
Values may be sent and summed in bfloat16 or wider, within the bound.
A program may use at most 192 MiB of HBM per device.

```python
import jax
import jax.numpy as jnp

EXPERTS = 16
D_MODEL = 4096
D_EXPERT = 6400


def raised(drawn, rng, source, target, parts, factor):
    def block_of(position):
        return (jnp.arange(drawn.shape[position]) // (drawn.shape[position] // parts)).reshape((-1,) + (1,) * (drawn.ndim - 1 - position))

    first = jax.random.permutation(rng, parts)[block_of(target)]
    other_side = (block_of(target) + parts // 2) % parts
    return jnp.where((block_of(source) == first) | (block_of(source) == other_side), factor * drawn, drawn)


def level_of(rng, shape, pieces, least, high):
    factor_of, own = 1.0, jax.random.fold_in(rng, 6)
    for dim, parts in pieces:
        heights = jnp.exp(jax.random.uniform(jax.random.fold_in(own, dim), (parts,), jnp.float32, least / len(pieces), high / len(pieces)))
        factor_of = factor_of * jnp.repeat(heights, shape[dim] // parts).reshape([-1 if axis == dim else 1 for axis in range(len(shape))])
    return factor_of


def normal_values(key, shape, width, bound, split=(), held_as=jnp.bfloat16):
    result = width * jax.random.normal(key, shape, jnp.float32)
    if split:
        result = result * level_of(key, shape, split, -0.22, 0.18)
    return jnp.clip(result, -bound, bound).astype(held_as)


def noise_with(key, dims, spread, most, cuts, heavy, kind=jnp.bfloat16):
    result = spread * jax.random.normal(key, dims, jnp.float32)
    if cuts:
        result = result * level_of(key, dims, cuts, -0.22, 0.18)
    return jnp.clip(raised(result, jax.random.fold_in(key, 3), *heavy), -most, most).astype(kind)


def setup_inputs(seed: int = 0) -> dict:
    streams_of = jax.random.split(jax.random.key(seed), 4)
    train_down = noise_with(streams_of[0], (EXPERTS, D_EXPERT, D_MODEL), D_EXPERT ** -0.5, 0.109375, ((0, 8), (2, 4)), (2, 1, 4, 2.0), jnp.float32)
    router_weight = normal_values(streams_of[1], (D_MODEL, EXPERTS), D_MODEL ** -0.5, 0.09375, ((0, 4), (1, 8)), jnp.float32)
    router_gain = jnp.clip(1.0 + 0.15 * jax.random.normal(streams_of[2], (D_MODEL,), jnp.float32), 0.25, 1.75)
    return dict(train_down=train_down, router_weight=router_weight, router_gain=router_gain)


def reference(train_down, router_weight, router_gain):
    scale_down = jnp.max(jnp.abs(train_down), axis=2)
    ready_down = (train_down / jnp.expand_dims(scale_down, 2)).astype(jnp.bfloat16)
    serve_router = (router_weight * router_gain[:, None]).astype(jnp.bfloat16)
    return ready_down, scale_down, serve_router
```

```python
import functools

import jax
import jax.numpy as jnp
from jax import lax
from jax.experimental import pallas as pl
from jax.experimental.pallas import tpu as pltpu
from jax.sharding import PartitionSpec as P

LANES = 128
TAIL_STEPS = 2
SLOTS = 4


def rows_per_step(count, n):
    fits = [r for r in range(16, count + 1, 16) if count % r == 0 and (n * r) % LANES == 0]
    wide = [r for r in fits if n * r >= 512]
    return wide[0] if wide else fits[-1]


def exchange_kernel(
    n, ne, rows, tail, x_hbm, weight_ref, gain_ref, *rest
):
    main_hbm, tails = rest[0], rest[1 : 1 + n]
    scale_ref, router_ref = rest[1 + n : 3 + n]
    (xbuf, narrow, own_max, seen_max, load_sem, max_send, max_recv,
     data_send, data_recv, keep_sem, router_sem) = rest[3 + n :]
    experts, all_rows, width = x_hbm.shape
    count = all_rows // n
    blocks = count // rows
    steps = experts * blocks
    groups = n * rows // LANES
    me = lax.axis_index("shard")
    mine = lax.axis_index("expert")

    def load(i, t):
        e, b = i // blocks, i % blocks
        return pltpu.make_async_copy(
            x_hbm.at[e, pl.ds(t * count + b * rows, rows), :],
            xbuf.at[i % SLOTS, pl.ds(t * rows, rows), :],
            load_sem.at[i % SLOTS],
        )

    def start_load(i):
        for t in range(n):
            load(i, t).start()

    start_load(0)
    start_load(1)

    barrier = pltpu.get_barrier_semaphore()
    for k in range(1, n):
        pl.semaphore_signal(barrier, inc=1, device_id={"shard": lax.rem(me + k, n)}, device_id_type=pl.DeviceIdType.MESH)
    for k in range(1, ne):
        pl.semaphore_signal(barrier, inc=1, device_id={"expert": lax.rem(mine + k, ne)}, device_id_type=pl.DeviceIdType.MESH)

    own_max[...] = jnp.zeros_like(own_max)
    router_ref[mine, me] = (weight_ref[...] * gain_ref[...]).astype(jnp.bfloat16)

    def local_max(i):
        slot = i % SLOTS
        pltpu.make_async_copy(xbuf.at[slot], xbuf.at[slot], load_sem.at[slot]).wait()
        for g in range(groups):
            at = pl.ds(g * LANES, LANES)
            top = jnp.abs(xbuf[slot, at, 0:LANES])
            for c in range(LANES, width, LANES):
                top = jnp.maximum(top, jnp.abs(xbuf[slot, at, c : c + LANES]))
            own_max[i, g : g + 1, :] = jnp.max(top.T, axis=0, keepdims=True)

    def max_copy(i, k):
        return pltpu.make_async_remote_copy(
            src_ref=own_max.at[i],
            dst_ref=seen_max.at[i, k - 1],
            send_sem=max_send.at[0],
            recv_sem=max_recv.at[i],
            device_id={"shard": lax.rem(me + k, n)},
            device_id_type=pl.DeviceIdType.MESH,
        )

    def divide(j):
        slot = j % SLOTS
        pltpu.make_async_copy(seen_max.at[j], seen_max.at[j], max_recv.at[j]).wait()
        full = own_max[j]
        for k in range(1, n):
            full = jnp.maximum(full, seen_max[j, k - 1])
        scale_ref[j] = full
        for g in range(groups):
            at = pl.ds(g * LANES, LANES)
            column = jnp.broadcast_to(full[g : g + 1, :], (LANES, LANES)).T
            for c in range(0, width, LANES):
                narrow[j, at, c : c + LANES] = (xbuf[slot, at, c : c + LANES] / column).astype(jnp.bfloat16)

    def block_of(j, k):
        target = lax.rem(me + k, n)
        return narrow.at[j, pl.ds(pl.multiple_of(target * rows, rows), rows), :]

    def send(j):
        e, b = j // blocks, j % blocks
        at = pl.ds(pl.multiple_of(b * rows, rows), rows)
        for k in range(1, n):
            pltpu.make_async_remote_copy(
                src_ref=block_of(j, k),
                dst_ref=main_hbm.at[k, e, at, :],
                send_sem=data_send.at[k],
                recv_sem=data_recv.at[k],
                device_id={"shard": lax.rem(me + k, n)},
                device_id_type=pl.DeviceIdType.MESH,
            ).start()
        pltpu.make_async_copy(block_of(j, 0), main_hbm.at[0, e, at, :], keep_sem.at[0]).start()

    def hand_over(j):
        for k in range(n):
            pltpu.make_async_copy(block_of(j, k), tails[k].at[j - (steps - tail)], keep_sem.at[1 + k]).start()

    local_max(0)
    pl.semaphore_wait(barrier, n - 1 + ne - 1)
    for k in range(1, n):
        max_copy(0, k).start()

    def step(i, carry):
        @pl.when(i + 1 < steps)
        def _():
            start_load(i + 1)

        local_max(i)
        divide(i - 1)
        for k in range(1, n):
            max_copy(i, k).start()

        @pl.when(i - 1 < steps - tail)
        def _():
            send(i - 1)

        @pl.when(i - 1 >= steps - tail)
        def _():
            hand_over(i - 1)

        return carry

    lax.fori_loop(1, steps, step, 0)
    divide(steps - 1)
    hand_over(steps - 1)

    for k in range(1, n):
        pltpu.make_async_remote_copy(
            src_ref=router_ref.at[mine, me], dst_ref=router_ref.at[mine, me],
            send_sem=router_sem.at[0], recv_sem=router_sem.at[1],
            device_id={"shard": lax.rem(me + k, n)}, device_id_type=pl.DeviceIdType.MESH,
        ).start()
    pieces = router_ref.at[mine, 0 : n - 1]
    pltpu.make_async_copy(pieces, pieces, router_sem.at[0]).wait()
    pltpu.make_async_copy(pieces, pieces, router_sem.at[1]).wait()
    for k in range(1, ne):
        pltpu.make_async_remote_copy(
            src_ref=router_ref.at[mine], dst_ref=router_ref.at[mine],
            send_sem=router_sem.at[2], recv_sem=router_sem.at[3],
            device_id={"expert": lax.rem(mine + k, ne)}, device_id_type=pl.DeviceIdType.MESH,
        ).start()
    slabs = router_ref.at[0 : ne - 1]
    pltpu.make_async_copy(slabs, slabs, router_sem.at[2]).wait()
    pltpu.make_async_copy(slabs, slabs, router_sem.at[3]).wait()

    for _ in range(1, n):
        every = own_max
        pltpu.make_async_copy(every, every, max_send.at[0]).wait()
    for k in range(n):
        pltpu.make_async_copy(tails[k], tails[k], keep_sem.at[1 + k]).wait()
    sent = narrow.at[0 : steps - tail, 0:rows, :]
    pltpu.make_async_copy(sent, sent, keep_sem.at[0]).wait()
    for k in range(1, n):
        pltpu.make_async_copy(sent, sent, data_send.at[k]).wait()
    for k in range(1, n):
        pltpu.make_async_copy(sent, sent, data_recv.at[k]).wait()


def place_kernel(n, position, *refs):
    parts, out_ref = refs[:n], refs[-1]
    width = parts[0].shape[-1]
    for k in range(n):
        source = lax.rem(position[0] - k + n, n)
        out_ref[0, :, pl.ds(pl.multiple_of(source * width, LANES), width)] = parts[k][...].reshape(out_ref.shape[1], width)


def per_device(n, ne, train_down, router_weight, router_gain):
    experts, all_rows, width = train_down.shape
    count = all_rows // n
    rows = rows_per_step(count, n)
    blocks = count // rows
    steps = experts * blocks
    tail = min(TAIL_STEPS, blocks)
    groups = n * rows // LANES
    padded = -(-groups // 8) * 8
    depth, columns = router_weight.shape
    bf16, f32 = jnp.bfloat16, jnp.float32
    hbm = pl.BlockSpec(memory_space=pl.ANY)
    vmem = pl.BlockSpec(memory_space=pltpu.VMEM)
    dma = pltpu.SemaphoreType.DMA
    results = pl.pallas_call(
        functools.partial(exchange_kernel, n, ne, rows, tail),
        out_shape=[jax.ShapeDtypeStruct((n, experts, count, width), bf16)]
        + [jax.ShapeDtypeStruct((tail, rows, width), bf16)] * n
        + [
            jax.ShapeDtypeStruct((steps, padded, LANES), f32),
            jax.ShapeDtypeStruct((ne, n, columns, depth), bf16),
        ],
        in_specs=[hbm, vmem, vmem],
        out_specs=[hbm] * (n + 1) + [vmem, vmem],
        scratch_shapes=[
            pltpu.VMEM((SLOTS, n * rows, width), f32),
            pltpu.VMEM((steps, n * rows, width), bf16),
            pltpu.VMEM((steps, padded, LANES), f32),
            pltpu.VMEM((steps, n - 1, padded, LANES), f32),
            dma((SLOTS,)),
            dma((1,)),
            dma((steps,)),
            dma((n,)),
            dma((n,)),
            dma((n + 1,)),
            dma((4,)),
        ],
        compiler_params=pltpu.CompilerParams(
            collective_id=0, has_side_effects=True, vmem_limit_bytes=56 * 1024 * 1024
        ),
        name="exchange",
    )(train_down, router_weight.T, router_gain[None, :])
    main, tails, scales, router = results[0], results[1 : 1 + n], results[1 + n], results[2 + n]

    moved = [tails[0]] + [
        lax.ppermute(tails[k], "shard", [(s, (s + k) % n) for s in range(n)]) for k in range(1, n)
    ]
    position = lax.axis_index("shard").astype(jnp.int32)[None]
    done = steps - tail

    def spot(i, position):
        return (i // blocks, i % blocks, 0)

    def part_spec(k):
        return pl.BlockSpec((1, 1, rows, width), lambda i, position: (k, i // blocks, i % blocks, 0))

    ready_shape = jax.ShapeDtypeStruct((experts, count, n * width), bf16)
    ready = pl.pallas_call(
        functools.partial(place_kernel, n),
        out_shape=ready_shape,
        grid_spec=pltpu.PrefetchScalarGridSpec(
            num_scalar_prefetch=1,
            grid=(done,),
            in_specs=[part_spec(k) for k in range(n)],
            out_specs=pl.BlockSpec((1, rows, n * width), spot),
        ),
        cost_estimate=pl.CostEstimate(flops=0, bytes_accessed=4 * done * n * rows * width, transcendentals=0),
        name="place_main",
    )(position, *([main] * n))

    ready_down = pl.pallas_call(
        functools.partial(place_kernel, n),
        out_shape=ready_shape,
        grid_spec=pltpu.PrefetchScalarGridSpec(
            num_scalar_prefetch=1,
            grid=(tail,),
            in_specs=[pl.BlockSpec((1, rows, width), lambda i, position: (i, 0, 0))] * n
            + [pl.BlockSpec(memory_space=pl.ANY)],
            out_specs=pl.BlockSpec((1, rows, n * width), lambda i, position: spot(i + done, position)),
        ),
        input_output_aliases={n + 1: 0},
        cost_estimate=pl.CostEstimate(flops=0, bytes_accessed=4 * tail * n * rows * width, transcendentals=0),
        name="place_tail",
    )(position, *moved, ready)

    by_target = scales[:, :groups, :].reshape(experts, blocks, n, rows)
    scale_down = lax.dynamic_index_in_dim(by_target, position[0], 2, keepdims=False).reshape(experts, count)
    serve_router = router.transpose(0, 2, 1, 3).reshape(ne * columns, n * depth).T
    return (ready_down, scale_down, serve_router)


def solution(mesh):
    in_specs = (P("expert", None, "shard"), P("shard", "expert"), P("shard"))
    out_specs = (P("expert", "shard", None), P("expert", "shard"), P())
    return jax.shard_map(
        functools.partial(per_device, mesh.shape["shard"], mesh.shape["expert"]),
        mesh=mesh, in_specs=in_specs, out_specs=out_specs, check_vma=False,
    )
```

```python
import functools

import jax
import jax.numpy as jnp
from jax import lax
from jax.experimental import pallas as pl
from jax.experimental.pallas import tpu as pltpu
from jax.sharding import PartitionSpec as P

LANES = 128
TAIL_SPAN = 320
MIN_SPAN = 640
LEAD = 7


def rows_per_step(count, n):
    fits = [r for r in range(16, count + 1, 16) if count % r == 0 and (n * r) % LANES == 0]
    wide = [r for r in fits if n * r >= MIN_SPAN]
    return wide[0] if wide else fits[-1]


def exchange_kernel(
    n, ne, rows, tail, lead, x_hbm, weight_ref, gain_ref, *rest
):
    main_hbm, tails = rest[0], rest[1 : 1 + n]
    scale_ref, router_ref = rest[1 + n : 3 + n]
    (xbuf, narrow, own_max, seen_max, load_sem, max_send, max_recv,
     data_send, data_recv, keep_sem, router_sem) = rest[3 + n :]
    experts, all_rows, width = x_hbm.shape
    count = all_rows // n
    blocks = count // rows
    steps = experts * blocks
    groups = n * rows // LANES
    me = lax.axis_index("shard")
    mine = lax.axis_index("expert")

    def load(i, t):
        e, b = i // blocks, i % blocks
        return pltpu.make_async_copy(
            x_hbm.at[e, pl.ds(t * count + b * rows, rows), :],
            xbuf.at[i % (lead + 3), pl.ds(t * rows, rows), :],
            load_sem.at[i % (lead + 3)],
        )

    def start_load(i):
        for t in range(n):
            load(i, t).start()

    start_load(0)
    start_load(1)

    barrier = pltpu.get_barrier_semaphore()
    for k in range(1, n):
        pl.semaphore_signal(barrier, inc=1, device_id={"shard": lax.rem(me + k, n)}, device_id_type=pl.DeviceIdType.MESH)
    for k in range(1, ne):
        pl.semaphore_signal(barrier, inc=1, device_id={"expert": lax.rem(mine + k, ne)}, device_id_type=pl.DeviceIdType.MESH)

    router_ref[mine, me] = (weight_ref[...] * gain_ref[...]).astype(jnp.bfloat16)

    def local_max(i):
        @pl.when(i + 2 < steps)
        def _():
            start_load(i + 2)

        slot = i % (lead + 3)
        pltpu.make_async_copy(xbuf.at[slot], xbuf.at[slot], load_sem.at[slot]).wait()
        for g in range(groups):
            at = pl.ds(g * LANES, LANES)
            top = jnp.abs(xbuf[slot, at, 0:LANES])
            for c in range(LANES, width, LANES):
                top = jnp.maximum(top, jnp.abs(xbuf[slot, at, c : c + LANES]))
            own_max[i, :, at] = jnp.max(top.T, axis=0, keepdims=True)

    def max_copy(i, k):
        return pltpu.make_async_remote_copy(
            src_ref=own_max.at[i],
            dst_ref=seen_max.at[i, k - 1],
            send_sem=max_send.at[0],
            recv_sem=max_recv.at[i],
            device_id={"shard": lax.rem(me + k, n)},
            device_id_type=pl.DeviceIdType.MESH,
        )

    def divide(j):
        slot = j % (lead + 3)
        pltpu.make_async_copy(seen_max.at[j], seen_max.at[j], max_recv.at[j]).wait()
        full = own_max[j]
        for k in range(1, n):
            full = jnp.maximum(full, seen_max[j, k - 1])
        scale_ref[j] = full
        for g in range(groups):
            at = pl.ds(g * LANES, LANES)
            column = jnp.broadcast_to(full[:, g * LANES : (g + 1) * LANES], (LANES, LANES)).T
            for c in range(0, width, LANES):
                narrow[j, at, c : c + LANES] = (xbuf[slot, at, c : c + LANES] / column).astype(jnp.bfloat16)

    def block_of(j, k):
        target = lax.rem(me + k, n)
        return narrow.at[j, pl.ds(pl.multiple_of(target * rows, rows), rows), :]

    def send(j):
        e, b = j // blocks, j % blocks
        at = pl.ds(pl.multiple_of(b * rows, rows), rows)
        for k in range(1, n):
            pltpu.make_async_remote_copy(
                src_ref=block_of(j, k),
                dst_ref=main_hbm.at[k, e, at, :],
                send_sem=data_send.at[k],
                recv_sem=data_recv.at[k],
                device_id={"shard": lax.rem(me + k, n)},
                device_id_type=pl.DeviceIdType.MESH,
            ).start()
        pltpu.make_async_copy(block_of(j, 0), main_hbm.at[0, e, at, :], keep_sem.at[0]).start()

    def hand_over(j):
        for k in range(n):
            pltpu.make_async_copy(block_of(j, k), tails[k].at[j - (steps - tail)], keep_sem.at[1 + k]).start()

    def send_max(i):
        for k in range(1, n):
            max_copy(i, k).start()

    def dispatch(j):
        @pl.when(j < steps - tail)
        def _():
            send(j)

        @pl.when(j >= steps - tail)
        def _():
            hand_over(j)

    def opening(j, carry):
        local_max(2 * j)
        local_max(2 * j + 1)
        send_max(2 * j)
        divide(j)
        send_max(2 * j + 1)
        dispatch(j)
        return carry

    def steady(j, carry):
        @pl.when(j + lead < steps)
        def _():
            local_max(j + lead)

        divide(j)

        @pl.when(j + lead < steps)
        def _():
            send_max(j + lead)

        dispatch(j)
        return carry

    local_max(0)
    pl.semaphore_wait(barrier, n - 1 + ne - 1)
    send_max(0)
    local_max(1)
    divide(0)
    send_max(1)
    dispatch(0)
    lax.fori_loop(1, lead, opening, 0)
    lax.fori_loop(lead, steps, steady, 0)

    for k in range(1, n):
        pltpu.make_async_remote_copy(
            src_ref=router_ref.at[mine, me], dst_ref=router_ref.at[mine, me],
            send_sem=router_sem.at[0], recv_sem=router_sem.at[1],
            device_id={"shard": lax.rem(me + k, n)}, device_id_type=pl.DeviceIdType.MESH,
        ).start()
    pieces = router_ref.at[mine, 0 : n - 1]
    pltpu.make_async_copy(pieces, pieces, router_sem.at[0]).wait()
    pltpu.make_async_copy(pieces, pieces, router_sem.at[1]).wait()
    for k in range(1, ne):
        pltpu.make_async_remote_copy(
            src_ref=router_ref.at[mine], dst_ref=router_ref.at[mine],
            send_sem=router_sem.at[2], recv_sem=router_sem.at[3],
            device_id={"expert": lax.rem(mine + k, ne)}, device_id_type=pl.DeviceIdType.MESH,
        ).start()
    slabs = router_ref.at[0 : ne - 1]
    pltpu.make_async_copy(slabs, slabs, router_sem.at[2]).wait()
    pltpu.make_async_copy(slabs, slabs, router_sem.at[3]).wait()

    for _ in range(1, n):
        every = own_max
        pltpu.make_async_copy(every, every, max_send.at[0]).wait()
    for k in range(n):
        pltpu.make_async_copy(tails[k], tails[k], keep_sem.at[1 + k]).wait()
    sent = narrow.at[0 : steps - tail, 0:rows, :]
    pltpu.make_async_copy(sent, sent, keep_sem.at[0]).wait()
    for k in range(1, n):
        pltpu.make_async_copy(sent, sent, data_send.at[k]).wait()
    for k in range(1, n):
        pltpu.make_async_copy(sent, sent, data_recv.at[k]).wait()


def place_kernel(n, position, *refs):
    parts, out_ref = refs[:n], refs[-1]
    width = parts[0].shape[-1]
    for k in range(n):
        source = lax.rem(position[0] - k + n, n)
        out_ref[0, :, pl.ds(pl.multiple_of(source * width, LANES), width)] = parts[k][...].reshape(out_ref.shape[1], width)


def per_device(n, ne, train_down, router_weight, router_gain):
    experts, all_rows, width = train_down.shape
    count = all_rows // n
    rows = rows_per_step(count, n)
    blocks = count // rows
    steps = experts * blocks
    lead = min(LEAD, steps // 2)
    tail = min(max(1, TAIL_SPAN // rows), blocks)
    depth, columns = router_weight.shape
    bf16, f32 = jnp.bfloat16, jnp.float32
    hbm = pl.BlockSpec(memory_space=pl.ANY)
    vmem = pl.BlockSpec(memory_space=pltpu.VMEM)
    dma = pltpu.SemaphoreType.DMA
    results = pl.pallas_call(
        functools.partial(exchange_kernel, n, ne, rows, tail, lead),
        out_shape=[jax.ShapeDtypeStruct((n, experts, count, width), bf16)]
        + [jax.ShapeDtypeStruct((tail, rows, width), bf16)] * n
        + [
            jax.ShapeDtypeStruct((steps, 1, n * rows), f32),
            jax.ShapeDtypeStruct((ne, n, columns, depth), bf16),
        ],
        in_specs=[hbm, vmem, vmem],
        out_specs=[hbm] * (n + 1) + [vmem, vmem],
        scratch_shapes=[
            pltpu.VMEM((lead + 3, n * rows, width), f32),
            pltpu.VMEM((steps, n * rows, width), bf16),
            pltpu.VMEM((steps, 1, n * rows), f32),
            pltpu.VMEM((steps, n - 1, 1, n * rows), f32),
            dma((lead + 3,)),
            dma((1,)),
            dma((steps,)),
            dma((n,)),
            dma((n,)),
            dma((n + 1,)),
            dma((4,)),
        ],
        compiler_params=pltpu.CompilerParams(
            collective_id=0, has_side_effects=True, vmem_limit_bytes=60 * 1024 * 1024
        ),
        name="exchange",
    )(train_down, router_weight.T, router_gain[None, :])
    main, tails, scales, router = results[0], results[1 : 1 + n], results[1 + n], results[2 + n]

    moved = [tails[0]] + [
        lax.ppermute(tails[k], "shard", [(s, (s + k) % n) for s in range(n)]) for k in range(1, n)
    ]
    position = lax.axis_index("shard").astype(jnp.int32)[None]
    done = steps - tail

    def spot(i, position):
        return (i // blocks, i % blocks, 0)

    def part_spec(k):
        return pl.BlockSpec((1, 1, rows, width), lambda i, position: (k, i // blocks, i % blocks, 0))

    ready_shape = jax.ShapeDtypeStruct((experts, count, n * width), bf16)
    ready = pl.pallas_call(
        functools.partial(place_kernel, n),
        out_shape=ready_shape,
        grid_spec=pltpu.PrefetchScalarGridSpec(
            num_scalar_prefetch=1,
            grid=(done,),
            in_specs=[part_spec(k) for k in range(n)],
            out_specs=pl.BlockSpec((1, rows, n * width), spot),
        ),
        cost_estimate=pl.CostEstimate(flops=0, bytes_accessed=4 * done * n * rows * width, transcendentals=0),
        name="place_main",
    )(position, *([main] * n))

    ready_down = pl.pallas_call(
        functools.partial(place_kernel, n),
        out_shape=ready_shape,
        grid_spec=pltpu.PrefetchScalarGridSpec(
            num_scalar_prefetch=1,
            grid=(tail,),
            in_specs=[pl.BlockSpec((1, rows, width), lambda i, position: (i, 0, 0))] * n
            + [pl.BlockSpec(memory_space=pl.ANY)],
            out_specs=pl.BlockSpec((1, rows, n * width), lambda i, position: spot(i + done, position)),
        ),
        input_output_aliases={n + 1: 0},
        cost_estimate=pl.CostEstimate(flops=0, bytes_accessed=4 * tail * n * rows * width, transcendentals=0),
        name="place_tail",
    )(position, *moved, ready)

    by_target = scales.reshape(experts, blocks, n, rows)
    scale_down = lax.dynamic_index_in_dim(by_target, position[0], 2, keepdims=False).reshape(experts, count)
    serve_router = router.transpose(0, 2, 1, 3).reshape(ne * columns, n * depth).T
    return (ready_down, scale_down, serve_router)


def solution(mesh):
    in_specs = (P("expert", None, "shard"), P("shard", "expert"), P("shard"))
    out_specs = (P("expert", "shard", None), P("expert", "shard"), P())
    return jax.shard_map(
        functools.partial(per_device, mesh.shape["shard"], mesh.shape["expert"]),
        mesh=mesh, in_specs=in_specs, out_specs=out_specs, check_vma=False,
    )
```
